32 devices in a mesh: gx: 8 (over z, x), gy: 4 (over y, core).
Axes of the slice: x: 2, y: 2, z: 4, core: 2. Of those that a mesh axis runs over, the one named last changes fastest.
Arguments:
- right_side: float32 [8, 32, 64, 512], P(None, 'gx', 'gy'), may hold values from -6 to 6
- velocity: float32 [3, 32, 64, 512], P(None, 'gx', 'gy'), may hold values from -0.5 to 0.5
- reaction: float32 [32, 64, 512], P('gx', 'gy'), may hold values from 0.1 to 2
Outputs:
- solution: float32 [8, 32, 64, 512], P(None, 'gx', 'gy')
- residual: float32 [8, 32, 64, 512], P(None, 'gx', 'gy')
The draws below stay inside these ranges and needn't reach their ends.
All inputs are finite; a program needn't handle non-finite values.
Results may differ from the reference program's by a relative error of at most 0.00045.
Values sent between devices are 32-bit elements; how exact they have to be, the bound alone decides.
A program may use at most 64 MiB of HBM per device.

```python
import math
import jax
import jax.numpy as jnp
import numpy as np
from jax import lax

CZ = 512
NRHS = 8
S = 4
ITERS = 2
NX = 32
NY = 64


def block_scale(rng, dims, split, smallest, high):
    def one(axis_at, blocks):
        heights = jax.random.uniform(jax.random.fold_in(jax.random.fold_in(rng, 6), axis_at), (blocks,), jnp.float32, smallest / len(split), high / len(split))
        return jnp.repeat(jnp.exp(heights), dims[axis_at] // blocks).reshape((-1,) + (1,) * (len(dims) - axis_at - 1))

    factor_of = one(*split[0])
    for cut in split[1:]:
        factor_of = factor_of * one(*cut)
    return factor_of


def noise(rng, shape, width, bound, shards=(), kind=jnp.bfloat16):
    result = width * jax.random.normal(rng, shape, jnp.float32)
    if shards:
        result = result * block_scale(rng, shape, shards, -0.22, 0.18)
    return jnp.clip(result, -bound, bound).astype(kind)


def setup_inputs(seed: int = 0) -> dict:
    key_list = jax.random.split(jax.random.key(seed), 4)
    right_side = noise(key_list[0], (NRHS, NX, NY, CZ), 1.0, 6.0, ((1, 8), (2, 4)), jnp.float32)
    velocity = jnp.clip(jax.random.uniform(key_list[1], (3, NX, NY, CZ), jnp.float32, -0.5, 0.5) * block_scale(key_list[1], (3, NX, NY, CZ), ((1, 8), (2, 4)), -0.4, 0.0), -0.5, 0.5)
    reaction = jnp.clip(jnp.exp(math.log(2.0) - 2.9957323 * jax.random.uniform(key_list[2], (NX, NY, CZ), jnp.float32) ** block_scale(key_list[2], (NX, NY, CZ), ((0, 8), (1, 4)), -0.2, 0.2)), 0.1, 2.0)
    return dict(right_side=right_side, velocity=velocity, reaction=reaction)


def apply_padded(padded, velocity, reaction):
    center = padded[:, 1:-1, 1:-1, 1:-1]
    neighbours = (1.0 - velocity[0]) * padded[:, 2:, 1:-1, 1:-1]
    neighbours = neighbours + (1.0 + velocity[0]) * padded[:, :-2, 1:-1, 1:-1]
    neighbours = neighbours + (1.0 - velocity[1]) * padded[:, 1:-1, 2:, 1:-1]
    neighbours = neighbours + (1.0 + velocity[1]) * padded[:, 1:-1, :-2, 1:-1]
    neighbours = neighbours + (1.0 - velocity[2]) * padded[:, 1:-1, 1:-1, 2:]
    neighbours = neighbours + (1.0 + velocity[2]) * padded[:, 1:-1, 1:-1, :-2]
    return (6.0 + reaction) * center - neighbours

def krylov_tables(nrhs, degree):
    total = (degree + 1) * nrhs
    mixing = np.zeros((total, degree * nrhs), np.float32)
    for column in range(degree * nrhs):
        mixing[column, column] = 6.0
        mixing[column + nrhs, column] = 6.0
    starting = np.zeros((total, nrhs), np.float32)
    starting[:nrhs] = np.eye(nrhs, dtype=np.float32)
    lifting = np.zeros((total, degree * nrhs), np.float32)
    lifting[:degree * nrhs] = np.eye(degree * nrhs, dtype=np.float32)
    return (jnp.asarray(mixing, jnp.float32), jnp.asarray(starting, jnp.float32), jnp.asarray(lifting, jnp.float32))

def solve_step(gram, nrhs, degree):
    mixing, starting, lifting = krylov_tables(nrhs, degree)
    highest = lax.Precision.HIGHEST
    mixed = jnp.dot(mixing.T, gram, precision=highest)
    normal = jnp.dot(mixed, mixing, precision=highest)
    target = jnp.dot(mixed, starting, precision=highest)
    factor = jnp.linalg.cholesky(normal)
    middle = lax.linalg.triangular_solve(factor, target, left_side=True, lower=True)
    update = lax.linalg.triangular_solve(factor, middle, left_side=True, lower=True, transpose_a=True)
    residual_coef = starting - jnp.dot(mixing, update, precision=highest)
    solution_coef = jnp.dot(lifting, update, precision=highest)
    return jnp.concatenate([solution_coef, residual_coef], axis=1)

def reference(right_side, velocity, reaction):
    nrhs = right_side.shape[0]
    highest = lax.Precision.HIGHEST
    solution = jnp.zeros_like(right_side)
    residual = right_side
    for outer_step in range(ITERS):
        basis = [residual]
        for power_step in range(S):
            current = basis[-1]
            padded = jnp.pad(current, ((0, 0), (1, 1), (1, 1), (1, 1)))
            image = apply_padded(padded, velocity, reaction)
            basis.append((image - 6.0 * current) / 6.0)
        stacked = jnp.stack(basis).reshape((S + 1) * nrhs, -1)
        gram = lax.dot_general(stacked, stacked, (((1,), (1,)), ((), ())), precision=highest)
        coefs = solve_step(gram, nrhs, S)
        combined = lax.dot_general(coefs, stacked, (((0,), (0,)), ((), ())), precision=highest)
        solution = solution + combined[:nrhs].reshape(right_side.shape)
        residual = combined[nrhs:].reshape(right_side.shape)
    return (solution, residual)
```

```python
import functools

import jax
import jax.numpy as jnp
from jax import lax
from jax.experimental import pallas as pl
from jax.experimental.pallas import tpu as pltpu
from jax.sharding import PartitionSpec as P

S = 4
ITERS = 2
F32 = jnp.float32
BF16 = jnp.bfloat16
MESH = pl.DeviceIdType.MESH


def iota(shape, dim):
    return lax.broadcasted_iota(jnp.int32, shape, dim)


def split(value):
    high = value.astype(BF16)
    low = (value - high.astype(F32)).astype(BF16)
    return jnp.concatenate([high, low], axis=0)


def coefficients(gram):
    size = S * 8
    lane = iota((size, 128), 1)
    row = iota((size, 128), 0)
    mixed = 6.0 * (gram[:size] + gram[8:])
    normal = 6.0 * (mixed + pltpu.roll(mixed, 120, 1))
    target = pltpu.roll(mixed, size, 1)
    work = jnp.where(lane < size, normal, jnp.where(lane < size + 8, target, 0.0))
    for k in range(size):
        pivot = 1.0 / work[k : k + 1, k : k + 1]
        line = work[k : k + 1, :] * pivot
        column = work[:, k : k + 1]
        work = jnp.where(row == k, line, work - column * line)
    update = jnp.where(lane < 8, pltpu.roll(work, 128 - size, 1), 0.0)
    none = jnp.zeros((8, 128), F32)
    upper = jnp.concatenate([update, none], axis=0)
    lower = jnp.concatenate([none, update], axis=0)
    total = size + 8
    start = jnp.where((iota((total, 128), 0) == iota((total, 128), 1)) & (iota((total, 128), 1) < 8), 1.0, 0.0)
    rest = start - 6.0 * (upper + lower)
    return upper + pltpu.roll(rest, 8, 1)


def kernel(ngx, ngy, X, Y, Z, rhs_ref, cf_ref, sol_ref, res_ref, basis, parts, gs, ag, ar_y, ar_x, send, recv, sy_s, sy_r, sx_s, sx_r):
    ix = lax.axis_index("gx")
    iy = lax.axis_index("gy")
    sides = [
        (ix > 0, ix - 1, iy),
        (ix < ngx - 1, ix + 1, iy),
        (iy > 0, ix, iy - 1),
        (iy < ngy - 1, ix, iy + 1),
    ]

    def face(slot, side):
        return [
            basis.at[slot, 1, pl.ds(1, Y)],
            basis.at[slot, X, pl.ds(1, Y)],
            basis.at[slot, pl.ds(1, X), 1],
            basis.at[slot, pl.ds(1, X), Y],
        ][side]

    def halo(slot, side):
        return [
            basis.at[slot, 0, pl.ds(1, Y)],
            basis.at[slot, X + 1, pl.ds(1, Y)],
            basis.at[slot, pl.ds(1, X), 0],
            basis.at[slot, pl.ds(1, X), Y + 1],
        ][side]

    def copy(slot, side):
        return pltpu.make_async_remote_copy(
            src_ref=face(slot, side),
            dst_ref=halo(slot, side ^ 1),
            send_sem=send.at[slot, side],
            recv_sem=recv.at[slot, side ^ 1],
            device_id={"gx": sides[side][1], "gy": sides[side][2]},
            device_id_type=MESH,
        )

    def start_sends(slot):
        for side in range(4):
            @pl.when(sides[side][0])
            def _():
                copy(slot, side).start()

    def wait_recvs(slot):
        for side in range(4):
            @pl.when(sides[side][0])
            def _():
                pltpu.make_async_remote_copy(
                    src_ref=halo(slot, side),
                    dst_ref=halo(slot, side),
                    send_sem=send.at[slot, side],
                    recv_sem=recv.at[slot, side],
                    device_id={"gx": sides[side][1], "gy": sides[side][2]},
                    device_id_type=MESH,
                ).wait_recv()

    def wait_sends(slot):
        for side in range(4):
            @pl.when(sides[side][0])
            def _():
                copy(slot, side).wait_send()

    nslots = ITERS * (S + 1)

    @pl.loop(0, nslots)
    def _(slot):
        for side in range(4):
            @pl.when(jnp.logical_not(sides[side][0]))
            def _():
                @pl.loop(0, Y if side < 2 else X)
                def _(at):
                    where = [(0, at + 1), (X + 1, at + 1), (at + 1, 0), (at + 1, Y + 1)][side]
                    basis[slot, where[0], where[1]] = jnp.zeros((8, Z), F32)

    lane = iota((8, Z), 1)
    first = lane == 0
    last = lane == Z - 1

    def keep(slot, power, x, y, value):
        basis[slot, x, y] = value
        parts[(x - 1) * Y + y - 1, pl.ds(16 * power, 16)] = split(value)

    def site(slot, power, x, y):
        c = basis[slot, x, y]
        xp, xm = basis[slot, x + 1, y], basis[slot, x - 1, y]
        yp, ym = basis[slot, x, y + 1], basis[slot, x, y - 1]
        zp = jnp.where(last, 0.0, pltpu.roll(c, Z - 1, 1))
        zm = jnp.where(first, 0.0, pltpu.roll(c, 1, 1))
        cf = [cf_ref[x - 1, y - 1, d : d + 1, :] for d in range(4)]
        sums = (xp + xm) - cf[0] * (xp - xm)
        sums = sums + ((yp + ym) - cf[1] * (yp - ym))
        sums = sums + ((zp + zm) - cf[2] * (zp - zm))
        keep(slot + 1, power + 1, x, y, (cf[3] * c - sums) * (1.0 / 6.0))

    def inner(slot, power):
        @pl.loop(2, X)
        def _(x):
            @pl.loop(2, Y)
            def _(y):
                site(slot, power, x, y)

    def outer(slot, power):
        @pl.loop(1, Y + 1)
        def _(y):
            site(slot, power, 1, y)
            site(slot, power, X, y)

        @pl.loop(2, X)
        def _(x):
            site(slot, power, x, 1)
            site(slot, power, x, Y)

    def exchange(outer_step, axis, count, me, buf, send_sem, recv_sem):
        def to(d):
            there = lax.rem(me + d, count)
            return pltpu.make_async_remote_copy(
                src_ref=ag.at[outer_step, axis],
                dst_ref=buf.at[outer_step, me],
                send_sem=send_sem.at[outer_step, d],
                recv_sem=recv_sem.at[outer_step, me],
                device_id={("gy", "gx")[axis]: there},
                device_id_type=MESH,
            )

        for d in range(1, count):
            to(d).start()
        for d in range(1, count):
            source = lax.rem(me + d, count)
            pltpu.make_async_remote_copy(
                src_ref=ag.at[outer_step, axis],
                dst_ref=buf.at[outer_step, source],
                send_sem=send_sem.at[outer_step, d],
                recv_sem=recv_sem.at[outer_step, source],
                device_id={("gy", "gx")[axis]: source},
                device_id_type=MESH,
            ).wait_recv()
        buf[outer_step, me] = ag[outer_step, axis]
        total = buf[outer_step, 0]
        for at in range(1, count):
            total = total + buf[outer_step, at]
        for d in range(1, count):
            to(d).wait_send()
        return total

    def gram_of(outer_step):
        def add(at, total):
            block = parts[at]
            return total + lax.dot_general(block, block, (((1,), (1,)), ((), ())), preferred_element_type=F32)

        gs[...] = jnp.zeros_like(gs)
        gs[:, 0:80] = lax.fori_loop(0, X * Y, add, jnp.zeros((80, 80), F32))
        rows = jnp.concatenate([gs[16 * j : 16 * j + 8, :] + gs[16 * j + 8 : 16 * j + 16, :] for j in range(S + 1)], axis=0)
        lanes = iota((40, 128), 1)
        gram = jnp.zeros((40, 128), F32)
        both = rows + pltpu.roll(rows, 120, 1)
        for j in range(S + 1):
            moved = both if j == 0 else pltpu.roll(both, 128 - 8 * j, 1)
            gram = jnp.where((lanes >= 8 * j) & (lanes < 8 * j + 8), moved, gram)
        tail = jnp.concatenate([gram[32:40], jnp.zeros((8, 128), F32)], axis=0)
        ag[outer_step, 0] = gram[0:16] + pltpu.roll(gram[16:32], 40, 1) + pltpu.roll(tail, 80, 1)
        ag[outer_step, 1] = exchange(outer_step, 0, ngy, iy, ar_y, sy_s, sy_r)
        total = exchange(outer_step, 1, ngx, ix, ar_x, sx_s, sx_r)
        gram = jnp.concatenate([total, pltpu.roll(total, 88, 1), pltpu.roll(total, 48, 1)[:8]], axis=0)
        return jnp.where(lanes < 40, gram, 0.0)

    @pl.loop(0, X)
    def _(x):
        @pl.loop(0, Y)
        def _(y):
            keep(0, 0, x + 1, y + 1, rhs_ref[x, y])

    for outer_step in range(ITERS):
        base = outer_step * (S + 1)

        @pl.loop(0, S)
        def _(power):
            slot = base + power
            start_sends(slot)
            inner(slot, power)
            wait_recvs(slot)
            outer(slot, power)
            wait_sends(slot)

        coefs = coefficients(gram_of(outer_step))
        doubled = []
        for j in range(S + 1):
            doubled += [coefs[8 * j : 8 * j + 8], coefs[8 * j : 8 * j + 8]]
        doubled.append(jnp.zeros((48, 128), F32))
        turned = jnp.concatenate(doubled, axis=0).T
        left = split(turned[0:16])[:, 0:80]

        @pl.loop(0, X)
        def _(x):
            @pl.loop(0, Y)
            def _(y):
                both = jnp.dot(left, parts[x * Y + y], preferred_element_type=F32)
                sol = both[0:8] + both[16:24]
                res = both[8:16] + both[24:32]
                if outer_step == 0:
                    sol_ref[x, y] = sol
                else:
                    sol_ref[x, y] += sol
                if outer_step < ITERS - 1:
                    keep(base + S + 1, 0, x + 1, y + 1, res)
                else:
                    res_ref[x, y] = res


def local(ngx, ngy, right_side, velocity, reaction):
    nrhs, X, Y, Z = right_side.shape
    rhs = jnp.transpose(right_side, (1, 2, 0, 3))
    cf = jnp.transpose(jnp.concatenate([velocity, reaction[None]], axis=0), (1, 2, 0, 3))
    nslots = ITERS * (S + 1)
    vmem = pl.BlockSpec(memory_space=pltpu.VMEM)
    out = jax.ShapeDtypeStruct((X, Y, nrhs, Z), F32)
    sol, res = pl.pallas_call(
        functools.partial(kernel, ngx, ngy, X, Y, Z),
        out_shape=(out, out),
        in_specs=[vmem, vmem],
        out_specs=(vmem, vmem),
        scratch_shapes=[
            pltpu.VMEM((nslots, X + 2, Y + 2, nrhs, Z), F32),
            pltpu.VMEM((X * Y, 80, Z), BF16),
            pltpu.VMEM((80, 128), F32),
            pltpu.VMEM((ITERS, 2, 16, 128), F32),
            pltpu.VMEM((ITERS, ngy, 16, 128), F32),
            pltpu.VMEM((ITERS, ngx, 16, 128), F32),
            pltpu.SemaphoreType.DMA((nslots, 4)),
            pltpu.SemaphoreType.DMA((nslots, 4)),
            pltpu.SemaphoreType.DMA((ITERS, ngy)),
            pltpu.SemaphoreType.DMA((ITERS, ngy)),
            pltpu.SemaphoreType.DMA((ITERS, ngx)),
            pltpu.SemaphoreType.DMA((ITERS, ngx)),
        ],
        compiler_params=pltpu.CompilerParams(has_side_effects=True, vmem_limit_bytes=56 * 1024 * 1024),
    )(rhs, cf)
    return jnp.transpose(sol, (2, 0, 1, 3)), jnp.transpose(res, (2, 0, 1, 3))


def solution(mesh):
    in_specs = (P(None, "gx", "gy", None), P(None, "gx", "gy", None), P("gx", "gy", None))
    out_specs = (P(None, "gx", "gy", None), P(None, "gx", "gy", None))
    body = functools.partial(local, mesh.shape["gx"], mesh.shape["gy"])
    return jax.shard_map(body, mesh=mesh, in_specs=in_specs, out_specs=out_specs, check_vma=False)
```

```python
import functools

import jax
import jax.numpy as jnp
from jax import lax
from jax.experimental import pallas as pl
from jax.experimental.pallas import tpu as pltpu
from jax.sharding import PartitionSpec as P

S = 4
ITERS = 2
F32 = jnp.float32
BF16 = jnp.bfloat16
MESH = pl.DeviceIdType.MESH


def iota(shape, dim):
    return lax.broadcasted_iota(jnp.int32, shape, dim)


def split(value):
    high = value.astype(BF16)
    low = (value - high.astype(F32)).astype(BF16)
    return jnp.concatenate([high, low], axis=0)


def coefficients(gram):
    size = S * 8
    lane = iota((size, 128), 1)
    row = iota((size, 128), 0)
    mixed = 6.0 * (gram[:size] + gram[8:])
    normal = 6.0 * (mixed + pltpu.roll(mixed, 120, 1))
    target = pltpu.roll(mixed, size, 1)
    work = jnp.where(lane < size, normal, jnp.where(lane < size + 8, target, 0.0))
    for k in range(size):
        pivot = 1.0 / work[k : k + 1, k : k + 1]
        line = work[k : k + 1, :] * pivot
        column = work[:, k : k + 1]
        work = jnp.where(row == k, line, work - column * line)
    update = jnp.where(lane < 8, pltpu.roll(work, 128 - size, 1), 0.0)
    none = jnp.zeros((8, 128), F32)
    upper = jnp.concatenate([update, none], axis=0)
    lower = jnp.concatenate([none, update], axis=0)
    total = size + 8
    start = jnp.where((iota((total, 128), 0) == iota((total, 128), 1)) & (iota((total, 128), 1) < 8), 1.0, 0.0)
    rest = start - 6.0 * (upper + lower)
    return upper + pltpu.roll(rest, 8, 1)


def kernel(ngx, ngy, X1, Y1, Z, rhs_ref, cf1_ref, sol_ref, res_ref, cf_ref, acc, turn_s, turn_r, back_s, back_r, basis, parts, gs, ag, ar_y, ar_x, send, recv, sy_s, sy_r, sx_s, sx_r):
    ix = lax.axis_index("gx")
    iy = lax.axis_index("gy")
    X, Y = 2 * X1, Y1 // 2
    odd = lax.rem(ix, 2)
    partner = ix + 1 - 2 * odd
    half = lax.rem(ix + iy, 2)
    upper = half == 1
    mine, theirs = odd * X1, (1 - odd) * X1
    sides = [
        (ix > 1, ix - 2, iy),
        (ix < ngx - 2, ix + 2, iy),
        (upper | (iy > 0), jnp.where(upper, partner, ix), jnp.where(upper, iy, iy - 1)),
        (jnp.logical_not(upper) | (iy < ngy - 1), jnp.where(upper, ix, partner), jnp.where(upper, iy + 1, iy)),
    ]

    def swap(which):
        source, target = [
            (rhs_ref.at[:, pl.ds((1 - half) * Y, Y)], basis.at[0, pl.ds(1 + mine, X1), pl.ds(1, Y)]),
            (cf1_ref.at[:, pl.ds((1 - half) * Y, Y)], cf_ref.at[pl.ds(mine, X1)]),
        ][which]
        return pltpu.make_async_remote_copy(
            src_ref=source,
            dst_ref=target,
            send_sem=turn_s.at[which],
            recv_sem=turn_r.at[which],
            device_id={"gx": partner, "gy": iy},
            device_id_type=MESH,
        )

    def swapped(which):
        target = [basis.at[0, pl.ds(1 + theirs, X1), pl.ds(1, Y)], cf_ref.at[pl.ds(theirs, X1)]][which]
        pltpu.make_async_remote_copy(
            src_ref=target,
            dst_ref=target,
            send_sem=turn_s.at[which],
            recv_sem=turn_r.at[which],
            device_id={"gx": partner, "gy": iy},
            device_id_type=MESH,
        ).wait_recv()

    def back(which, plane):
        return pltpu.make_async_remote_copy(
            src_ref=acc.at[which, theirs + plane],
            dst_ref=[sol_ref, res_ref][which].at[plane, pl.ds(half * Y, Y)],
            send_sem=back_s.at[which, plane],
            recv_sem=back_r.at[which, plane],
            device_id={"gx": partner, "gy": iy},
            device_id_type=MESH,
        )

    def came_back(which, plane):
        target = [sol_ref, res_ref][which].at[plane, pl.ds((1 - half) * Y, Y)]
        pltpu.make_async_remote_copy(
            src_ref=target,
            dst_ref=target,
            send_sem=back_s.at[which, plane],
            recv_sem=back_r.at[which, plane],
            device_id={"gx": partner, "gy": iy},
            device_id_type=MESH,
        ).wait_recv()

    swap(0).start()
    swap(1).start()

    def face(slot, side):
        return [
            basis.at[slot, 1, pl.ds(1, Y)],
            basis.at[slot, X, pl.ds(1, Y)],
            basis.at[slot, pl.ds(1, X), 1],
            basis.at[slot, pl.ds(1, X), Y],
        ][side]

    def halo(slot, side):
        return [
            basis.at[slot, 0, pl.ds(1, Y)],
            basis.at[slot, X + 1, pl.ds(1, Y)],
            basis.at[slot, pl.ds(1, X), 0],
            basis.at[slot, pl.ds(1, X), Y + 1],
        ][side]

    def copy(slot, side):
        return pltpu.make_async_remote_copy(
            src_ref=face(slot, side),
            dst_ref=halo(slot, side ^ 1),
            send_sem=send.at[slot, side],
            recv_sem=recv.at[slot, side ^ 1],
            device_id={"gx": sides[side][1], "gy": sides[side][2]},
            device_id_type=MESH,
        )

    def start_sends(slot):
        for side in range(4):
            @pl.when(sides[side][0])
            def _():
                copy(slot, side).start()

    def wait_recvs(slot):
        for side in range(4):
            @pl.when(sides[side][0])
            def _():
                pltpu.make_async_remote_copy(
                    src_ref=halo(slot, side),
                    dst_ref=halo(slot, side),
                    send_sem=send.at[slot, side],
                    recv_sem=recv.at[slot, side],
                    device_id={"gx": sides[side][1], "gy": sides[side][2]},
                    device_id_type=MESH,
                ).wait_recv()

    def wait_sends(slot):
        for side in range(4):
            @pl.when(sides[side][0])
            def _():
                copy(slot, side).wait_send()

    nslots = ITERS * (S + 1)

    @pl.loop(0, nslots)
    def _(slot):
        for side in range(4):
            @pl.when(jnp.logical_not(sides[side][0]))
            def _():
                @pl.loop(0, Y if side < 2 else X)
                def _(at):
                    where = [(0, at + 1), (X + 1, at + 1), (at + 1, 0), (at + 1, Y + 1)][side]
                    basis[slot, where[0], where[1]] = jnp.zeros((8, Z), F32)

    lane = iota((8, Z), 1)
    first = lane == 0
    last = lane == Z - 1

    def keep(slot, power, x, y, value):
        basis[slot, x, y] = value
        parts[(x - 1) * Y + y - 1, pl.ds(16 * power, 16)] = split(value)

    def site(slot, power, x, y):
        c = basis[slot, x, y]
        xp, xm = basis[slot, x + 1, y], basis[slot, x - 1, y]
        yp, ym = basis[slot, x, y + 1], basis[slot, x, y - 1]
        zp = jnp.where(last, 0.0, pltpu.roll(c, Z - 1, 1))
        zm = jnp.where(first, 0.0, pltpu.roll(c, 1, 1))
        cf = [cf_ref[x - 1, y - 1, d : d + 1, :] for d in range(4)]
        sums = (xp + xm) - cf[0] * (xp - xm)
        sums = sums + ((yp + ym) - cf[1] * (yp - ym))
        sums = sums + ((zp + zm) - cf[2] * (zp - zm))
        keep(slot + 1, power + 1, x, y, (cf[3] * c - sums) * (1.0 / 6.0))

    def inner(slot, power):
        @pl.loop(2, X)
        def _(x):
            @pl.loop(2, Y, unroll=True)
            def _(y):
                site(slot, power, x, y)

    def outer(slot, power):
        @pl.loop(1, Y + 1, unroll=4)
        def _(y):
            site(slot, power, 1, y)
            site(slot, power, X, y)

        @pl.loop(2, X, unroll=True)
        def _(x):
            site(slot, power, x, 1)
            site(slot, power, x, Y)

    def exchange(outer_step, axis, count, me, buf, send_sem, recv_sem):
        def to(d):
            there = lax.rem(me + d, count)
            return pltpu.make_async_remote_copy(
                src_ref=ag.at[outer_step, axis],
                dst_ref=buf.at[outer_step, me],
                send_sem=send_sem.at[outer_step, d],
                recv_sem=recv_sem.at[outer_step, me],
                device_id={("gy", "gx")[axis]: there},
                device_id_type=MESH,
            )

        for d in range(1, count):
            to(d).start()
        for d in range(1, count):
            source = lax.rem(me + d, count)
            pltpu.make_async_remote_copy(
                src_ref=ag.at[outer_step, axis],
                dst_ref=buf.at[outer_step, source],
                send_sem=send_sem.at[outer_step, d],
                recv_sem=recv_sem.at[outer_step, source],
                device_id={("gy", "gx")[axis]: source},
                device_id_type=MESH,
            ).wait_recv()
        buf[outer_step, me] = ag[outer_step, axis]
        total = buf[outer_step, 0]
        for at in range(1, count):
            total = total + buf[outer_step, at]
        for d in range(1, count):
            to(d).wait_send()
        return total

    def gram_of(outer_step):
        def add(at, total):
            block = parts[at]
            return total + lax.dot_general(block, block, (((1,), (1,)), ((), ())), preferred_element_type=F32)

        gs[...] = jnp.zeros_like(gs)
        gs[:, 0:80] = lax.fori_loop(0, X * Y, add, jnp.zeros((80, 80), F32), unroll=8)
        rows = jnp.concatenate([gs[16 * j : 16 * j + 8, :] + gs[16 * j + 8 : 16 * j + 16, :] for j in range(S + 1)], axis=0)
        lanes = iota((40, 128), 1)
        gram = jnp.zeros((40, 128), F32)
        both = rows + pltpu.roll(rows, 120, 1)
        for j in range(S + 1):
            moved = both if j == 0 else pltpu.roll(both, 128 - 8 * j, 1)
            gram = jnp.where((lanes >= 8 * j) & (lanes < 8 * j + 8), moved, gram)
        tail = jnp.concatenate([gram[32:40], jnp.zeros((8, 128), F32)], axis=0)
        ag[outer_step, 0] = gram[0:16] + pltpu.roll(gram[16:32], 40, 1) + pltpu.roll(tail, 80, 1)
        ag[outer_step, 1] = exchange(outer_step, 0, ngy, iy, ar_y, sy_s, sy_r)
        total = exchange(outer_step, 1, ngx, ix, ar_x, sx_s, sx_r)
        gram = jnp.concatenate([total, pltpu.roll(total, 88, 1), pltpu.roll(total, 48, 1)[:8]], axis=0)
        return jnp.where(lanes < 40, gram, 0.0)

    @pl.loop(0, X1)
    def _(x):
        @pl.loop(0, Y, unroll=8)
        def _(y):
            keep(0, 0, mine + x + 1, y + 1, rhs_ref[x, half * Y + y])
            cf_ref[mine + x, y] = cf1_ref[x, half * Y + y]

    swapped(0)

    def split_swapped():
        @pl.loop(0, X1)
        def _(x):
            @pl.loop(0, Y, unroll=8)
            def _(y):
                parts[(theirs + x) * Y + y, pl.ds(0, 16)] = split(basis[0, theirs + x + 1, y + 1])

    for outer_step in range(ITERS):
        base = outer_step * (S + 1)

        @pl.loop(0, S)
        def _(power):
            slot = base + power
            start_sends(slot)
            if outer_step == 0:
                @pl.when(power == 0)
                def _():
                    split_swapped()
                    swapped(1)
            inner(slot, power)
            wait_recvs(slot)
            outer(slot, power)
            wait_sends(slot)

        coefs = coefficients(gram_of(outer_step))
        doubled = []
        for j in range(S + 1):
            doubled += [coefs[8 * j : 8 * j + 8], coefs[8 * j : 8 * j + 8]]
        doubled.append(jnp.zeros((48, 128), F32))
        turned = jnp.concatenate(doubled, axis=0).T
        left = split(turned[0:16])[:, 0:80]

        def combined(x, y):
            both = jnp.dot(left, parts[x * Y + y], preferred_element_type=F32)
            sol, res = both[0:8] + both[16:24], both[8:16] + both[24:32]
            return sol if outer_step == 0 else acc[0, x, y] + sol, res

        if outer_step < ITERS - 1:
            @pl.loop(0, X)
            def _(x):
                @pl.loop(0, Y, unroll=8)
                def _(y):
                    sol, res = combined(x, y)
                    acc[0, x, y] = sol
                    keep(base + S + 1, 0, x + 1, y + 1, res)
        else:
            @pl.loop(0, X1)
            def _(x):
                @pl.loop(0, Y, unroll=8)
                def _(y):
                    acc[0, theirs + x, y], acc[1, theirs + x, y] = combined(theirs + x, y)

                back(0, x).start()
                back(1, x).start()

            @pl.loop(0, X1)
            def _(x):
                @pl.loop(0, Y, unroll=8)
                def _(y):
                    sol, res = combined(mine + x, y)
                    sol_ref[x, half * Y + y] = sol
                    res_ref[x, half * Y + y] = res

            for which in range(2):
                swap(which).wait_send()

            @pl.loop(0, X1)
            def _(x):
                for which in range(2):
                    came_back(which, x)
                    back(which, x).wait_send()


def local(ngx, ngy, right_side, velocity, reaction):
    nrhs, X, Y, Z = right_side.shape
    rhs = jnp.transpose(right_side, (1, 2, 0, 3))
    cf = jnp.transpose(jnp.concatenate([velocity, reaction[None]], axis=0), (1, 2, 0, 3))
    nslots = ITERS * (S + 1)
    vmem = pl.BlockSpec(memory_space=pltpu.VMEM)
    out = jax.ShapeDtypeStruct((X, Y, nrhs, Z), F32)
    sol, res = pl.pallas_call(
        functools.partial(kernel, ngx, ngy, X, Y, Z),
        out_shape=(out, out),
        in_specs=[vmem, vmem],
        out_specs=(vmem, vmem),
        scratch_shapes=[
            pltpu.VMEM((2 * X, Y // 2, 4, Z), F32),
            pltpu.VMEM((2, 2 * X, Y // 2, nrhs, Z), F32),
            pltpu.SemaphoreType.DMA((2,)),
            pltpu.SemaphoreType.DMA((2,)),
            pltpu.SemaphoreType.DMA((2, X)),
            pltpu.SemaphoreType.DMA((2, X)),
            pltpu.VMEM((nslots, 2 * X + 2, Y // 2 + 2, nrhs, Z), F32),
            pltpu.VMEM((X * Y, 80, Z), BF16),
            pltpu.VMEM((80, 128), F32),
            pltpu.VMEM((ITERS, 2, 16, 128), F32),
            pltpu.VMEM((ITERS, ngy, 16, 128), F32),
            pltpu.VMEM((ITERS, ngx, 16, 128), F32),
            pltpu.SemaphoreType.DMA((nslots, 4)),
            pltpu.SemaphoreType.DMA((nslots, 4)),
            pltpu.SemaphoreType.DMA((ITERS, ngy)),
            pltpu.SemaphoreType.DMA((ITERS, ngy)),
            pltpu.SemaphoreType.DMA((ITERS, ngx)),
            pltpu.SemaphoreType.DMA((ITERS, ngx)),
        ],
        compiler_params=pltpu.CompilerParams(has_side_effects=True, vmem_limit_bytes=56 * 1024 * 1024),
    )(rhs, cf)
    return jnp.transpose(sol, (2, 0, 1, 3)), jnp.transpose(res, (2, 0, 1, 3))


def solution(mesh):
    in_specs = (P(None, "gx", "gy", None), P(None, "gx", "gy", None), P("gx", "gy", None))
    out_specs = (P(None, "gx", "gy", None), P(None, "gx", "gy", None))
    body = functools.partial(local, mesh.shape["gx"], mesh.shape["gy"])
    return jax.shard_map(body, mesh=mesh, in_specs=in_specs, out_specs=out_specs, check_vma=False)
```

```python
import functools

import jax
import jax.numpy as jnp
from jax import lax
from jax.experimental import pallas as pl
from jax.experimental.pallas import tpu as pltpu
from jax.sharding import PartitionSpec as P

S = 4
ITERS = 2
F32 = jnp.float32
BF16 = jnp.bfloat16
MESH = pl.DeviceIdType.MESH


def iota(shape, dim):
    return lax.broadcasted_iota(jnp.int32, shape, dim)


def split(value):
    high = value.astype(BF16)
    low = (value - high.astype(F32)).astype(BF16)
    return jnp.concatenate([high, low], axis=0)


def coefficients(gram):
    size = S * 8
    lane = iota((size, 128), 1)
    row = iota((size, 128), 0)
    mixed = 6.0 * (gram[:size] + gram[8:])
    normal = 6.0 * (mixed + pltpu.roll(mixed, 120, 1))
    target = pltpu.roll(mixed, size, 1)
    work = jnp.where(lane < size, normal, jnp.where(lane < size + 8, target, 0.0))
    for k in range(size):
        pivot = 1.0 / work[k : k + 1, k : k + 1]
        line = work[k : k + 1, :] * pivot
        column = work[:, k : k + 1]
        work = jnp.where(row == k, line, work - column * line)
    update = jnp.where(lane < 8, pltpu.roll(work, 128 - size, 1), 0.0)
    none = jnp.zeros((8, 128), F32)
    upper = jnp.concatenate([update, none], axis=0)
    lower = jnp.concatenate([none, update], axis=0)
    total = size + 8
    start = jnp.where((iota((total, 128), 0) == iota((total, 128), 1)) & (iota((total, 128), 1) < 8), 1.0, 0.0)
    rest = start - 6.0 * (upper + lower)
    return upper + pltpu.roll(rest, 8, 1)


def kernel(ngx, ngy, X1, Y1, Z, rhs_ref, vel_ref, rea_ref, sol_ref, res_ref, cf_ref, came, acc, gone, turn_s, turn_r, back_s, back_r, basis, parts, gs, ag, ar_y, ar_x, send, recv, sy_s, sy_r, sx_s, sx_r):
    ix = lax.axis_index("gx")
    iy = lax.axis_index("gy")
    X, Y = 2 * X1, Y1 // 2
    odd = lax.rem(ix, 2)
    partner = ix + 1 - 2 * odd
    half = lax.rem(ix + iy, 2)
    upper = half == 1
    mine, theirs = odd * X1, (1 - odd) * X1
    sides = [
        (ix > 1, ix - 2, iy),
        (ix < ngx - 2, ix + 2, iy),
        (upper | (iy > 0), jnp.where(upper, partner, ix), jnp.where(upper, iy, iy - 1)),
        (jnp.logical_not(upper) | (iy < ngy - 1), jnp.where(upper, ix, partner), jnp.where(upper, iy + 1, iy)),
    ]

    my_rows = pl.ds(pl.multiple_of(half * Y, Y), Y)
    their_rows = pl.ds(pl.multiple_of((1 - half) * Y, Y), Y)

    def swap(which):
        source, target = [
            (rhs_ref.at[:, :, their_rows], came),
            (vel_ref.at[:, :, their_rows], cf_ref.at[pl.ds(0, 3), pl.ds(mine, X1)]),
            (rea_ref.at[:, their_rows], cf_ref.at[3, pl.ds(mine, X1)]),
        ][which]
        return pltpu.make_async_remote_copy(
            src_ref=source,
            dst_ref=target,
            send_sem=turn_s.at[which],
            recv_sem=turn_r.at[which],
            device_id={"gx": partner, "gy": iy},
            device_id_type=MESH,
        )

    def swapped(which):
        target = [came, cf_ref.at[pl.ds(0, 3), pl.ds(theirs, X1)], cf_ref.at[3, pl.ds(theirs, X1)]][which]
        pltpu.make_async_remote_copy(
            src_ref=target,
            dst_ref=target,
            send_sem=turn_s.at[which],
            recv_sem=turn_r.at[which],
            device_id={"gx": partner, "gy": iy},
            device_id_type=MESH,
        ).wait_recv()

    def back(which, plane):
        return pltpu.make_async_remote_copy(
            src_ref=gone.at[which, plane],
            dst_ref=[sol_ref, res_ref][which].at[:, plane, my_rows],
            send_sem=back_s.at[which, plane],
            recv_sem=back_r.at[which, plane],
            device_id={"gx": partner, "gy": iy},
            device_id_type=MESH,
        )

    def came_back(which, plane):
        target = [sol_ref, res_ref][which].at[:, plane, their_rows]
        pltpu.make_async_remote_copy(
            src_ref=target,
            dst_ref=target,
            send_sem=back_s.at[which, plane],
            recv_sem=back_r.at[which, plane],
            device_id={"gx": partner, "gy": iy},
            device_id_type=MESH,
        ).wait_recv()

    swap(0).start()
    swap(1).start()
    swap(2).start()

    def face(slot, side):
        return [
            basis.at[slot, 1, pl.ds(1, Y)],
            basis.at[slot, X, pl.ds(1, Y)],
            basis.at[slot, pl.ds(1, X), 1],
            basis.at[slot, pl.ds(1, X), Y],
        ][side]

    def halo(slot, side):
        return [
            basis.at[slot, 0, pl.ds(1, Y)],
            basis.at[slot, X + 1, pl.ds(1, Y)],
            basis.at[slot, pl.ds(1, X), 0],
            basis.at[slot, pl.ds(1, X), Y + 1],
        ][side]

    def copy(slot, side):
        return pltpu.make_async_remote_copy(
            src_ref=face(slot, side),
            dst_ref=halo(slot, side ^ 1),
            send_sem=send.at[slot, side],
            recv_sem=recv.at[slot, side ^ 1],
            device_id={"gx": sides[side][1], "gy": sides[side][2]},
            device_id_type=MESH,
        )

    def start_sends(slot):
        for side in range(4):
            @pl.when(sides[side][0])
            def _():
                copy(slot, side).start()

    def wait_recvs(slot):
        for side in range(4):
            @pl.when(sides[side][0])
            def _():
                pltpu.make_async_remote_copy(
                    src_ref=halo(slot, side),
                    dst_ref=halo(slot, side),
                    send_sem=send.at[slot, side],
                    recv_sem=recv.at[slot, side],
                    device_id={"gx": sides[side][1], "gy": sides[side][2]},
                    device_id_type=MESH,
                ).wait_recv()

    def wait_sends(slot):
        for side in range(4):
            @pl.when(sides[side][0])
            def _():
                copy(slot, side).wait_send()

    nslots = ITERS * (S + 1)

    gs[...] = jnp.zeros_like(gs)

    @pl.loop(0, nslots)
    def _(slot):
        for side in range(4):
            @pl.when(jnp.logical_not(sides[side][0]))
            def _():
                @pl.loop(0, Y if side < 2 else X)
                def _(at):
                    where = [(0, at + 1), (X + 1, at + 1), (at + 1, 0), (at + 1, Y + 1)][side]
                    basis[slot, where[0], where[1]] = jnp.zeros((8, Z), F32)

    lane = iota((8, Z), 1)
    first = lane == 0
    last = lane == Z - 1

    def keep(slot, power, x, y, value):
        basis[slot, x, y] = value
        parts[(x - 1) * Y + y - 1, pl.ds(16 * power, 16)] = split(value)

    def site(slot, power, x, y):
        c = basis[slot, x, y]
        xp, xm = basis[slot, x + 1, y], basis[slot, x - 1, y]
        yp, ym = basis[slot, x, y + 1], basis[slot, x, y - 1]
        zp = jnp.where(last, 0.0, pltpu.roll(c, Z - 1, 1))
        zm = jnp.where(first, 0.0, pltpu.roll(c, 1, 1))
        cf = [cf_ref[d, x - 1, y - 1 : y, :] for d in range(4)]
        sums = (xp + xm) - cf[0] * (xp - xm)
        sums = sums + ((yp + ym) - cf[1] * (yp - ym))
        sums = sums + ((zp + zm) - cf[2] * (zp - zm))
        keep(slot + 1, power + 1, x, y, (cf[3] * c - sums) * (1.0 / 6.0))

    def inner(slot, power):
        @pl.loop(2, X)
        def _(x):
            for y in range(2, Y):
                site(slot, power, x, y)

    def outer(slot, power):
        @pl.loop(0, 2)
        def _(end):
            for y in range(1, Y + 1):
                site(slot, power, 1 + end * (X - 1), y)

        @pl.loop(2, X, unroll=True)
        def _(x):
            site(slot, power, x, 1)
            site(slot, power, x, Y)

    def exchange(outer_step, axis, count, me, buf, send_sem, recv_sem):
        def to(d):
            there = lax.rem(me + d, count)
            return pltpu.make_async_remote_copy(
                src_ref=ag.at[outer_step, axis],
                dst_ref=buf.at[outer_step, me],
                send_sem=send_sem.at[outer_step, d],
                recv_sem=recv_sem.at[outer_step, me],
                device_id={("gy", "gx")[axis]: there},
                device_id_type=MESH,
            )

        for d in range(1, count):
            to(d).start()
        for d in range(1, count):
            source = lax.rem(me + d, count)
            pltpu.make_async_remote_copy(
                src_ref=ag.at[outer_step, axis],
                dst_ref=buf.at[outer_step, source],
                send_sem=send_sem.at[outer_step, d],
                recv_sem=recv_sem.at[outer_step, source],
                device_id={("gy", "gx")[axis]: source},
                device_id_type=MESH,
            ).wait_recv()
        buf[outer_step, me] = ag[outer_step, axis]
        total = buf[outer_step, 0]
        for at in range(1, count):
            total = total + buf[outer_step, at]
        for d in range(1, count):
            to(d).wait_send()
        return total

    low = 16 * S

    def gram_low():
        def add(at, total):
            block = parts[at, 0:low]
            return total + lax.dot_general(block, block, (((1,), (1,)), ((), ())), preferred_element_type=F32)

        gs[0:low, 0:low] = lax.fori_loop(0, X * Y, add, jnp.zeros((low, low), F32), unroll=8)

    def gram_of(outer_step):
        def add(at, total):
            return total + lax.dot_general(
                parts[at], parts[at, low : low + 16], (((1,), (1,)), ((), ())), preferred_element_type=F32
            )

        gs[:, low : low + 16] = lax.fori_loop(0, X * Y, add, jnp.zeros((low + 16, 16), F32), unroll=8)
        rows = jnp.concatenate([gs[16 * j : 16 * j + 8, :] + gs[16 * j + 8 : 16 * j + 16, :] for j in range(S + 1)], axis=0)
        lanes = iota((40, 128), 1)
        gram = jnp.zeros((40, 128), F32)
        both = rows + pltpu.roll(rows, 120, 1)
        for j in range(S + 1):
            moved = both if j == 0 else pltpu.roll(both, 128 - 8 * j, 1)
            gram = jnp.where((lanes >= 8 * j) & (lanes < 8 * j + 8), moved, gram)
        tail = jnp.concatenate([gram[32:40], jnp.zeros((8, 128), F32)], axis=0)
        ag[outer_step, 0] = gram[0:16] + pltpu.roll(gram[16:32], 40, 1) + pltpu.roll(tail, 80, 1)
        ag[outer_step, 1] = exchange(outer_step, 0, ngy, iy, ar_y, sy_s, sy_r)
        total = exchange(outer_step, 1, ngx, ix, ar_x, sx_s, sx_r)
        gram = jnp.concatenate([total, pltpu.roll(total, 88, 1), pltpu.roll(total, 48, 1)[:8]], axis=0)
        gram = jnp.where(lanes < 40, gram, 0.0)
        turned = jnp.concatenate([gram, jnp.zeros((88, 128), F32)], axis=0).T[32:40]
        turned = jnp.where(iota((8, 128), 1) < 32, turned, gram[32:40])
        return jnp.concatenate([gram[:32], turned], axis=0)

    def place(x, fields):
        turned = jnp.swapaxes(fields, 0, 1)
        for y in range(Y):
            keep(0, 0, x + 1, y + 1, turned[y])

    @pl.loop(0, X1)
    def _(x):
        place(mine + x, rhs_ref[:, x, my_rows, :])
        for d in range(3):
            cf_ref[d, mine + x] = vel_ref[d, x, my_rows, :]
        cf_ref[3, mine + x] = rea_ref[x, my_rows, :]

    swapped(0)

    @pl.loop(0, X1)
    def _(x):
        place(theirs + x, came[:, x])

    for outer_step in range(ITERS):
        base = outer_step * (S + 1)

        @pl.loop(0, S)
        def _(power):
            slot = base + power
            start_sends(slot)
            if outer_step == 0:
                @pl.when(power == 0)
                def _():
                    swapped(1)
                    swapped(2)
            inner(slot, power)

            @pl.when(power == S - 1)
            def _():
                gram_low()

            wait_recvs(slot)
            outer(slot, power)
            wait_sends(slot)

        coefs = coefficients(gram_of(outer_step))
        doubled = []
        for j in range(S + 1):
            doubled += [coefs[8 * j : 8 * j + 8], coefs[8 * j : 8 * j + 8]]
        doubled.append(jnp.zeros((48, 128), F32))
        turned = jnp.concatenate(doubled, axis=0).T
        left = split(turned[0:16])[:, 0:80]

        def combined(x, y):
            both = jnp.dot(left, parts[x * Y + y], preferred_element_type=F32)
            sol, res = both[0:8] + both[16:24], both[8:16] + both[24:32]
            return sol if outer_step == 0 else acc[x, y] + sol, res

        def plane(x):
            both = [combined(x, y) for y in range(Y)]
            return tuple(jnp.swapaxes(jnp.stack([one[k] for one in both]), 0, 1) for k in range(2))

        if outer_step < ITERS - 1:
            @pl.loop(0, X)
            def _(x):
                @pl.loop(0, Y, unroll=8)
                def _(y):
                    sol, res = combined(x, y)
                    acc[x, y] = sol
                    keep(base + S + 1, 0, x + 1, y + 1, res)
        else:
            @pl.loop(0, X1)
            def _(x):
                sol, res = plane(theirs + x)
                gone[0, x] = sol
                gone[1, x] = res
                back(0, x).start()
                back(1, x).start()

            @pl.loop(0, X1)
            def _(x):
                sol, res = plane(mine + x)
                sol_ref[:, x, my_rows, :] = sol
                res_ref[:, x, my_rows, :] = res

            for which in range(3):
                swap(which).wait_send()

            @pl.loop(0, X1)
            def _(x):
                for which in range(2):
                    came_back(which, x)
                    back(which, x).wait_send()


def local(ngx, ngy, right_side, velocity, reaction):
    nrhs, X, Y, Z = right_side.shape
    nslots = ITERS * (S + 1)
    vmem = pl.BlockSpec(memory_space=pltpu.VMEM)
    out = jax.ShapeDtypeStruct(right_side.shape, F32)
    return pl.pallas_call(
        functools.partial(kernel, ngx, ngy, X, Y, Z),
        out_shape=(out, out),
        in_specs=[vmem, vmem, vmem],
        out_specs=(vmem, vmem),
        scratch_shapes=[
            pltpu.VMEM((4, 2 * X, Y // 2, Z), F32),
            pltpu.VMEM((nrhs, X, Y // 2, Z), F32),
            pltpu.VMEM((2 * X, Y // 2, nrhs, Z), F32),
            pltpu.VMEM((2, X, nrhs, Y // 2, Z), F32),
            pltpu.SemaphoreType.DMA((3,)),
            pltpu.SemaphoreType.DMA((3,)),
            pltpu.SemaphoreType.DMA((2, X)),
            pltpu.SemaphoreType.DMA((2, X)),
            pltpu.VMEM((nslots, 2 * X + 2, Y // 2 + 2, nrhs, Z), F32),
            pltpu.VMEM((X * Y, 80, Z), BF16),
            pltpu.VMEM((80, 128), F32),
            pltpu.VMEM((ITERS, 2, 16, 128), F32),
            pltpu.VMEM((ITERS, ngy, 16, 128), F32),
            pltpu.VMEM((ITERS, ngx, 16, 128), F32),
            pltpu.SemaphoreType.DMA((nslots, 4)),
            pltpu.SemaphoreType.DMA((nslots, 4)),
            pltpu.SemaphoreType.DMA((ITERS, ngy)),
            pltpu.SemaphoreType.DMA((ITERS, ngy)),
            pltpu.SemaphoreType.DMA((ITERS, ngx)),
            pltpu.SemaphoreType.DMA((ITERS, ngx)),
        ],
        compiler_params=pltpu.CompilerParams(has_side_effects=True, vmem_limit_bytes=56 * 1024 * 1024),
    )(right_side, velocity, reaction)


def solution(mesh):
    in_specs = (P(None, "gx", "gy", None), P(None, "gx", "gy", None), P("gx", "gy", None))
    out_specs = (P(None, "gx", "gy", None), P(None, "gx", "gy", None))
    body = functools.partial(local, mesh.shape["gx"], mesh.shape["gy"])
    return jax.shard_map(body, mesh=mesh, in_specs=in_specs, out_specs=out_specs, check_vma=False)
```
